32 devices in a mesh: groups: 2 (over y), ep: 4 (over z), dp: 4 (over x, core), tp: 1.
Axes of the slice: x: 2, y: 2, z: 4, core: 2. Of those that a mesh axis runs over, the one named last changes fastest.
Arguments:
- tokens: bfloat16 [2048, 2048], P(('groups', 'ep', 'dp', 'tp')), parts along dimension 0, may hold values from -6 to 6
- experts_one: int32 [2048, 8], P(('groups', 'ep', 'dp', 'tp')), parts along dimension 0, may hold values from 0 to 15, all different within a row; in each aligned block of 64 rows (0 to 63, 64 to 127, ...) at most 40 rows name the same one
- gates_one: float32 [2048, 8], P(('groups', 'ep', 'dp', 'tp')), parts along dimension 0, may hold values from 0.05 to 0.5
- w_in_one: bfloat16 [16, 2048, 2, 768], P(('ep', 'dp'), None, None, 'tp'), may hold values from -0.125 to 0.125
- w_down_one: bfloat16 [16, 768, 2048], P(('ep', 'dp'), 'tp'), may hold values from -0.21875 to 0.21875
- norm_gain: float32 [2048], replicated, may hold values from 0.5 to 1.5
- experts_two: int32 [2048, 8], P(('groups', 'ep', 'dp', 'tp')), parts along dimension 0, may hold values from 0 to 15, all different within a row; in each aligned block of 64 rows (0 to 63, 64 to 127, ...) at most 40 rows name the same one
- gates_two: float32 [2048, 8], P(('groups', 'ep', 'dp', 'tp')), parts along dimension 0, may hold values from 0.05 to 0.5
- placement_two: int32 [16], replicated, may hold values from 0 to 15, each once
- w_in_two: bfloat16 [16, 2048, 2, 768], P(('ep', 'dp'), None, None, 'tp'), may hold values from -0.125 to 0.125
- w_down_two: bfloat16 [16, 768, 2048], P(('ep', 'dp'), 'tp'), may hold values from -0.21875 to 0.21875
Outputs:
- layer_out: bfloat16 [2048, 2048], P(('groups', 'ep', 'dp', 'tp')), parts along dimension 0
The draws below stay inside these ranges and needn't reach their ends.
There are 2 independent parts, one for each index of `groups`. The reference program is written for one: setup_inputs(seed, part) draws one part's arguments, and reference() takes and returns one part's arrays. A program takes and returns all parts, laid end to end along the dimension named above; an argument that names none is the same for every part. Nothing has to cross between parts.
Inputs may be any that keep to these rules, and one draw needn't show every extreme that they name: `experts_one`: each token names 8 different experts; among the 64 tokens of one device no expert is named more than 40 times, and on some device some expert is named exactly 40 times. `experts_two`: each token names 8 different experts; among the 64 tokens of one device no expert is named more than 40 times, and on some device some expert is named exactly 40 times. `placement_two`: each slot is named by exactly one expert.
All inputs are finite; a program needn't handle non-finite values.
Results may differ from the reference program's by a relative error of at most 0.011.
Values may be sent and summed in bfloat16 or wider, within the bound.
A program may use at most 128 MiB of HBM per device.

```python
import math
import jax
import jax.numpy as jnp
import numpy as np
from jax import lax

D = 2048
FF = 768
TOPK = 8
TOK_DEV = 64
EXPERTS = 16
MOST = 40
TOKENS = 1024
N_EP = 4
N_DP = 4
N_TP = 1


def shard_levels(key, dims, cuts, smallest, top_value):
    loudness, own = 1.0, jax.random.fold_in(key, 6)
    for position, parts in cuts:
        heights = jnp.exp(jax.random.uniform(jax.random.fold_in(own, position), (parts,), jnp.float32, smallest / len(cuts), top_value / len(cuts)))
        loudness = loudness * jnp.repeat(heights, dims[position] // parts).reshape([-1 if axis == position else 1 for axis in range(len(dims))])
    return loudness


def assign_block(stream_key, own, number, rows, count, top, limit, lean):
    sequence = jax.random.permutation(stream_key, count)
    crowded, common = shares(count, rows * top, limit, lean, True), shares(count, rows * top, limit, lean, False)
    places = jnp.arange(count)

    def named(sizes, rotation):
        used = int((sizes > 0).sum())
        fixed = max(1, used // 4)
        passed = fixed + (places - fixed + rotation * (used - fixed)) % max(1, count - fixed)
        return jnp.zeros((count,), jnp.int32).at[sequence[jnp.where(places < fixed, places, passed)]].set(jnp.asarray(sizes, jnp.int32))

    sizes = jnp.where(number % 4 == 0, named(crowded, number // 4), named(common, number - number // 4 - 1))
    mixed = jax.random.permutation(jax.random.fold_in(own, 3), count)
    giver, receiver = mixed[0:count // 2 * 2:2], mixed[1:count // 2 * 2:2]
    margin = jnp.minimum(sizes[giver] - 1, limit - sizes[receiver]) // 2
    margin = jnp.where((giver == sequence[0]) | (receiver == sequence[0]) | (sizes[receiver] == 0), 0, jnp.maximum(margin, 0))
    passed = jax.random.randint(jax.random.fold_in(own, 4), (count // 2,), 0, 1 << 20) % (margin + 1)
    sizes = sizes.at[giver].add(-passed).at[receiver].add(passed)
    labels = jnp.searchsorted(jnp.cumsum(sizes), jnp.arange(rows * top), side="right").astype(jnp.int32)
    listing = labels.reshape(top, rows).T
    listing = listing[jax.random.permutation(jax.random.fold_in(own, 1), rows)]
    rotation = jax.random.randint(jax.random.fold_in(own, 2), (rows, 1), 0, top)
    return jnp.take_along_axis(listing, (jnp.arange(top)[None, :] + rotation) % top, axis=1)


def shares(count, total, bound, lean, full):
    weights = [(1 << 20) // math.isqrt(rank ** lean) + 1 for rank in range(1, count + 1)]
    largest = bound if full else min(bound, max(-(-total // count), total * weights[0] // sum(weights)))
    least = 1 if total - largest >= count - 1 else 0
    holding, spare = [largest] + [least] * (count - 1), total - largest - least * (count - 1)
    while spare > 0:
        candidates = [i for i in range(1, count) if holding[i] < largest] or [i for i in range(1, count) if holding[i] < bound]
        whole, remaining = sum([weights[i] for i in candidates]), spare
        for i in candidates:
            more = min(bound - holding[i], max(1, remaining * weights[i] // whole), spare)
            holding[i] = holding[i] + more
            spare = spare - more
    return np.array(holding)


def gaussian(own_key, extent, scale, reach, cuts=(), kind=jnp.bfloat16):
    entries = jax.random.normal(own_key, extent, jnp.float32) * scale
    if len(cuts) > 0:
        entries = shard_levels(own_key, extent, cuts, -0.22, 0.18) * entries
    return jnp.clip(entries, min=-reach, max=reach).astype(kind)


def setup_inputs(seed: int = 0, part: int = 0) -> dict:
    key_of = jax.random.split(jax.random.key(seed), 12)
    part_splits = jax.random.split(jax.random.fold_in(key_of[11], part), 12)
    tokens = gaussian(part_splits[0], (TOKENS, D), 1.0, 6.0, ((0, 16),))
    experts_one_keys = jax.random.split(jax.random.fold_in(part_splits[1], 1), TOKENS // TOK_DEV)
    experts_one_turns = jax.random.permutation(jax.random.fold_in(part_splits[1], 3), TOKENS // TOK_DEV)
    experts_one = jax.vmap(lambda own, number: assign_block(jax.random.fold_in(part_splits[1], 2), own, number, TOK_DEV, EXPERTS, TOPK, MOST, 2))(experts_one_keys, experts_one_turns).reshape((TOKENS, TOPK))
    gates_one = jnp.clip(jnp.exp(math.log(0.5) - 2.3025851 * jax.random.uniform(part_splits[2], (TOKENS, TOPK), jnp.float32) ** shard_levels(part_splits[2], (TOKENS, TOPK), ((0, 16),), -0.2, 0.2)), 0.05, 0.5)
    w_in_one = gaussian(key_of[3], (EXPERTS, D, 2, FF), D ** -0.5, 0.125, ((0, 16),))
    w_down_one = gaussian(key_of[4], (EXPERTS, FF, D), FF ** -0.5, 0.21875, ((0, 16),))
    norm_gain = jnp.clip(1.0 + 0.1 * jax.random.normal(key_of[5], (D,), jnp.float32), 0.5, 1.5)
    experts_two_keys = jax.random.split(jax.random.fold_in(part_splits[6], 1), TOKENS // TOK_DEV)
    experts_two_turns = jax.random.permutation(jax.random.fold_in(part_splits[6], 3), TOKENS // TOK_DEV)
    experts_two = jax.vmap(lambda own, number: assign_block(jax.random.fold_in(part_splits[6], 2), own, number, TOK_DEV, EXPERTS, TOPK, MOST, 2))(experts_two_keys, experts_two_turns).reshape((TOKENS, TOPK))
    gates_two = jnp.clip(jnp.exp(math.log(0.5) - 2.3025851 * jax.random.uniform(part_splits[7], (TOKENS, TOPK), jnp.float32) ** shard_levels(part_splits[7], (TOKENS, TOPK), ((0, 16),), -0.2, 0.2)), 0.05, 0.5)
    placement_two = jax.random.permutation(key_of[8], EXPERTS).astype(jnp.int32)
    w_in_two = gaussian(key_of[9], (EXPERTS, D, 2, FF), D ** -0.5, 0.125, ((0, 16),))
    w_down_two = gaussian(key_of[10], (EXPERTS, FF, D), FF ** -0.5, 0.21875, ((0, 16),))
    return dict(tokens=tokens, experts_one=experts_one, gates_one=gates_one, w_in_one=w_in_one, w_down_one=w_down_one, norm_gain=norm_gain, experts_two=experts_two, gates_two=gates_two, placement_two=placement_two, w_in_two=w_in_two, w_down_two=w_down_two)


def expert_layer(rows_in, layer_slots, gate_values, w_in, w_down):
    token_count, top_count = layer_slots.shape
    expert_total, row_width, pair_n, hidden_n = w_in.shape
    slot_cap = MOST * N_EP * N_DP * N_TP
    block_width = hidden_n // N_TP
    flat_ids = layer_slots.reshape(-1)
    owner_row = jnp.arange(token_count * top_count, dtype=jnp.int32) // top_count
    flat_gates = gate_values.reshape(-1)

    def accumulate(summed, expert_id):
        hit_mask = flat_ids == expert_id
        slot_rank = jnp.cumsum(hit_mask.astype(jnp.int32)) - 1
        slot_pos = jnp.where(hit_mask, slot_rank, slot_cap).astype(jnp.int32)
        picked = jnp.zeros((slot_cap,), jnp.int32).at[slot_pos].set(owner_row, mode='drop')
        weight = jnp.zeros((slot_cap,), jnp.float32).at[slot_pos].set(flat_gates, mode='drop')
        chosen = rows_in[picked]
        gate_up = jnp.dot(chosen, w_in[expert_id].reshape(row_width, pair_n * hidden_n), preferred_element_type=jnp.float32)
        activated = (jax.nn.silu(gate_up[:, :hidden_n]) * gate_up[:, hidden_n:]).astype(jnp.bfloat16)
        down_now = w_down[expert_id]
        total = jnp.zeros((slot_cap, row_width), jnp.float32)
        for block in range(N_TP):
            lo_unit = block * block_width
            partial_out = jnp.dot(activated[:, lo_unit:lo_unit + block_width], down_now[lo_unit:lo_unit + block_width], preferred_element_type=jnp.float32)
            total = total + partial_out.astype(jnp.bfloat16).astype(jnp.float32)
        expert_out = total.astype(jnp.bfloat16)
        summed = summed.at[picked].add(weight[:, None] * expert_out.astype(jnp.float32))
        return (summed, None)
    start_sum = jnp.zeros((token_count, row_width), jnp.float32)
    summed, _ = lax.scan(accumulate, start_sum, jnp.arange(expert_total, dtype=jnp.int32))
    return summed

def reference(tokens, experts_one, gates_one, w_in_one, w_down_one, norm_gain, experts_two, gates_two, placement_two, w_in_two, w_down_two):
    moe_one = expert_layer(tokens, experts_one, gates_one, w_in_one, w_down_one)
    mixed = (tokens.astype(jnp.float32) + moe_one).astype(jnp.bfloat16)
    mixed = lax.optimization_barrier(mixed)
    mixed_wide = mixed.astype(jnp.float32)
    inv_rms = lax.rsqrt(lax.optimization_barrier(jnp.mean(mixed_wide * mixed_wide, axis=1, keepdims=True)) + 1e-06)
    normed = (mixed_wide * inv_rms * norm_gain[None, :]).astype(jnp.bfloat16)
    layer_slots = placement_two[experts_two].astype(jnp.int32)
    moe_two = expert_layer(normed, layer_slots, gates_two, w_in_two, w_down_two)
    return (mixed_wide + moe_two).astype(jnp.bfloat16)
```

```python
import functools

import jax
import jax.numpy as jnp
from jax import lax
from jax.experimental import pallas as pl
from jax.experimental.pallas import tpu as pltpu
from jax.sharding import PartitionSpec as P

MESH = pl.DeviceIdType.MESH
LANES = 128


STREAMS = 2
PIECES = 2
GATHER = ('zx', 'zx')
REDUCE = ('zz', 'zz')
PROGRAM = (
    "S00 W0 S01 W1",
    "x000 a002 a001 x010",
    "a011 C000 a003 x002",
    "C010 k000 C002 x001",
    "b012 k010 b011 x003",
    "k002 a012 C001 C003",
    "a013 C012 k003 b013",
    "t002 k012 k001 C013",
    "t003 C011 t012 t000",
    "k013 t001 k011 t013",
    "F00 t011 t010 a101",
    "x100 a102 F01 x101",
    "C101 x102 a103 C100",
    "x110 C102 x103 k101",
    "a111 a112 k100 C103",
    "b112 k103 a113 b111",
    "C112 k102 b113 t103",
    "k112 C113 t102 t101",
    "k113 C111 C110 k111",
    "t100 t113 k110 t112",
    "t111 F10 t110 F11",
)


def fused_kernel(
    n, experts, width, tokens_hbm, experts_hbm, gates_hbm, experts2_hbm, gates2_hbm, gain_ref, place, w_in1, w_down1,
    w_in2, w_down2, out, tokens, ids, gates, mixed, rows1, rows2, part, core_in, cross, x_in, z_in, raw, w_in, w_down,
    hidden, w_sem, z_send, z_recv, x_send, x_recv, c_send, c_recv, rc_send, rc_recv, rx_send, rx_recv, rz_send, rz_recv,
):
    z = lax.axis_index("ep")
    d = lax.axis_index("dp")
    mine = z * lax.axis_size("dp") + d
    x_peer = {"dp": (d + 2) % 4}
    c_peer = {"dp": d + 1 - 2 * (d % 2)}
    half = w_down.shape[1]
    tok = tokens.shape[0]
    size = tok // STREAMS
    pair = z + 1 - 2 * (z % 2)
    other = 3 - z
    order = [z, pair, 2 - z // 2, 3 - 3 * (z // 2)]
    inner = z % 3 != 0
    outer = jnp.logical_not(inner)
    rows = [rows1, rows2]
    f32, bf16 = jnp.float32, jnp.bfloat16
    cut = size // PIECES
    at = [pl.ds(p * cut, cut) for p in range(PIECES)]

    def remote(src, dst, send, recv, to):
        return pltpu.make_async_remote_copy(
            src_ref=src, dst_ref=dst, send_sem=send, recv_sem=recv, device_id=to, device_id_type=MESH
        )

    small = [
        pltpu.make_async_copy(src, dst, w_sem.at[k])
        for k, (src, dst) in enumerate(
            [
                (tokens_hbm, tokens), (experts_hbm, ids.at[0]), (gates_hbm, gates.at[0]),
                (experts2_hbm, ids.at[1]), (gates2_hbm, gates.at[1]),
            ]
        )
    ]
    load_in = [pltpu.make_async_copy(w, raw, w_sem.at[5 + k]) for k, w in enumerate((w_in1, w_in2))]
    load_down = [pltpu.make_async_copy(w, w_down.at[k], w_sem.at[7 + k]) for k, w in enumerate((w_down1, w_down2))]
    for copy in small + [load_in[0], load_down[0], load_down[1]]:
        copy.start()

    barrier = pltpu.get_barrier_semaphore()
    pl.semaphore_signal(barrier, inc=1, device_id={"ep": pair}, device_id_type=MESH)
    pl.semaphore_signal(barrier, inc=1, device_id=x_peer, device_id_type=MESH)
    pl.semaphore_signal(barrier, inc=1, device_id=c_peer, device_id_type=MESH)

    @pl.when(inner)
    def _():
        pl.semaphore_signal(barrier, inc=1, device_id={"ep": other}, device_id_type=MESH)

    sends = []

    def go(copy, when=None):
        if when is None:
            copy.start()
        else:
            pl.when(when)(copy.start)
        sends.append((copy, when))

    for copy in small:
        copy.wait()
    lane = lax.broadcasted_iota(jnp.int32, (LANES, tok), 0)
    table = jnp.zeros((LANES, tok), f32)
    for l in range(2):
        here = jnp.where(lane // (2 * experts) == l, lane % experts, -1)
        for k in range(ids.shape[1]):
            table += jnp.where(ids[l, k : k + 1] == here, gates[l, k : k + 1], 0.0)
    high = table.astype(bf16).astype(f32)
    table = jnp.where((lane // experts) % 2 == 0, high, table - high).T.astype(bf16)
    for s in range(STREAMS):
        own = pl.ds(s * size, size)
        rows1[s, z, 0, :, :width] = tokens[own]
        rows1[s, z, 0, :, width:] = table[s * size : (s + 1) * size]
    e_mine = 0
    for e in range(experts):
        e_mine = e_mine + jnp.where(place[e] == mine, e, 0)
    lanes = [mine, 2 * experts + e_mine]

    @pl.when(inner)
    def _():
        pl.semaphore_wait(barrier, 4)

    @pl.when(outer)
    def _():
        pl.semaphore_wait(barrier, 3)

    def block(l, s, b, j):
        return rows[l].at[s, b, j]

    def z_own(l, s, j):
        q = 2 * l + s
        for p in range(PIECES):
            spot = block(l, s, z, j).at[at[p]]
            up = remote(spot, spot, z_send.at[q, 0, j, p], z_recv.at[q, z, j, p], {"ep": pair})
            go(up)
            down = remote(spot, spot, z_send.at[q, 1, j, p], z_recv.at[q, z, j, p], {"ep": other})
            go(down, inner)

    def x_move(l, s, i):
        q, b = 2 * l + s, order[i]
        for p in range(PIECES):
            go(
                remote(
                    block(l, s, b, 0).at[at[p]], block(l, s, b, 1).at[at[p]], x_send.at[q, i, p], x_recv.at[q, i, p], x_peer
                )
            )

    def c_move(l, s, i, j):
        q, b = 2 * l + s, order[i]
        go(remote(block(l, s, b, j), block(l, s, b, 2 + j), c_send.at[q, i, j], c_recv.at[q, i, j], c_peer))

    def start(l, s):
        z_own(l, s, 0)
        x_move(l, s, 0)
        c_move(l, s, 0, 0)

    def arrive(j, l, s, i):
        q, b = 2 * l + s, order[i]
        to = {"ep": other if i == 1 else pair}
        first = GATHER[l][s] == "z"
        if first and j == 1:
            return
        for p in range(PIECES):
            spot = block(l, s, b, j).at[at[p]]
            move = remote(spot, spot, z_send.at[q, 1 + i, j, p], z_recv.at[q, b, j, p], to)
            move.wait_recv()
            go(move, inner)
            if first:
                go(
                    remote(spot, block(l, s, b, 1).at[at[p]], x_send.at[q, i, p], x_recv.at[q, i, p], x_peer)
                )
        c_move(l, s, i, j)

    def x_arrive(l, s, i):
        if GATHER[l][s] == "x" and i > 0:
            return
        q, b = 2 * l + s, order[i]
        for p in range(PIECES):
            spot = block(l, s, b, 1).at[at[p]]
            remote(spot, spot, x_send.at[q, i, p], x_recv.at[q, i, p], x_peer).wait_recv()
        if GATHER[l][s] == "x":
            z_own(l, s, 1)
        c_move(l, s, i, 1)

    def weights(l):
        load_in[l].wait()
        group = 128

        @pl.loop(0, width // group)
        def _(j):
            here = pl.ds(pl.multiple_of(j * group, group), group)
            w_in[l, here] = raw[here].reshape(group, 2 * half)

        load_down[l].wait()
        if l == 0:
            load_in[1].start()

    def compute(l, s, i):
        q, b = 2 * l + s, order[i]
        for j in range(2):
            spot = block(l, s, b, 2 + j)
            remote(spot, spot, c_send.at[q, i, j], c_recv.at[q, i, j], c_peer).wait_recv()
        count = 4 * size
        marks = rows1[s, b, :, :, width:].reshape(count, LANES).astype(f32)
        spots = lax.broadcasted_iota(jnp.int32, (count, LANES), 1)
        hit = (spots == lanes[l]) | (spots == lanes[l] + experts)
        weight = jnp.sum(jnp.where(hit, marks, 0.0), axis=1, keepdims=True)
        step = half

        @pl.loop(0, half // step)
        def _(j):
            x = rows[l][s, b, :, :, :width].reshape(count, width)
            here = pl.multiple_of(j * step, step)
            gate = jnp.dot(x, w_in[l, :, pl.ds(here, step)], preferred_element_type=f32)
            up = jnp.dot(x, w_in[l, :, pl.ds(half + here, step)], preferred_element_type=f32)
            hidden[:, pl.ds(here, step)] = (gate / (1.0 + jnp.exp(-gate)) * up).astype(bf16)

        y = jnp.dot(hidden[...], w_down[l], preferred_element_type=f32)
        y = jnp.where(weight == 0.0, 0.0, y * weight)
        part[q, i] = y.astype(bf16).reshape(4, size, width)
        go(remote(part.at[q, i, pl.ds(2, 2)], core_in.at[q, i], rc_send.at[q, i], rc_recv.at[q, i], c_peer))

    def pair_sum(q, i, j, p):
        return part[q, i, j, at[p]].astype(f32) + core_in[q, i, j, at[p]].astype(f32)

    def z_wait(q, slot, j, p):
        spot = z_in.at[q, slot, j, at[p]]
        remote(spot, spot, rz_send.at[q, 0, j, p], rz_recv.at[q, slot, j, p], {"ep": pair}).wait_recv()

    def line(q, i, j, p, value):
        slot_in = {1: 4, 2: 2, 3: 3}[i]
        slot_inner = {1: 0, 2: 1, 3: 4}[i]
        slot_outer = {1: 0, 2: 2, 3: 3}[i]
        slot = slot_inner if slot_inner == slot_outer else jnp.where(inner, slot_inner, slot_outer)
        to = pair if i == 1 else jnp.where(inner, other, pair)

        @pl.when(inner)
        def _():
            z_wait(q, slot_in, j, p)
            cross[q, i, j, at[p]] = (value() + z_in[q, slot_in, j, at[p]].astype(f32)).astype(bf16)

        @pl.when(outer)
        def _():
            cross[q, i, j, at[p]] = value().astype(bf16)

        go(
            remote(
                cross.at[q, i, j, at[p]], z_in.at[q, slot, j, at[p]], rz_send.at[q, i, j, p], rz_recv.at[q, slot, j, p],
                {"ep": to},
            )
        )

    def rx_go(q, i, p):
        go(
            remote(cross.at[q, i, 1, at[p]], x_in.at[q, i, at[p]], rx_send.at[q, i, p], rx_recv.at[q, i, p], x_peer)
        )

    def rx_wait(q, i, p):
        spot = x_in.at[q, i, at[p]]
        remote(spot, spot, rx_send.at[q, i, p], rx_recv.at[q, i, p], x_peer).wait_recv()

    def core_arrive(l, s, i):
        q = 2 * l + s
        remote(core_in.at[q, i], core_in.at[q, i], rc_send.at[q, i], rc_recv.at[q, i], c_peer).wait_recv()
        if REDUCE[l][s] == "z":
            for p in range(PIECES):
                cross[q, i, 1, at[p]] = pair_sum(q, i, 1, p).astype(bf16)
                rx_go(q, i, p)

    def total(j, l, s, i):
        q = 2 * l + s
        if REDUCE[l][s] == "z":
            for p in range(PIECES if j == 0 else 0):
                rx_wait(q, i, p)
                if i > 0:
                    line(q, i, 0, p, lambda: pair_sum(q, i, 0, p) + x_in[q, i, at[p]].astype(f32))
        elif i > 0:
            for p in range(PIECES):
                line(q, i, j, p, lambda: pair_sum(q, i, j, p))

    def gathered(q, j, p, value):
        z_wait(q, 0, j, p)
        pl.when(inner)(functools.partial(z_wait, q, 1, j, p))
        value = value + z_in[q, 0, j, at[p]].astype(f32)
        return value + jnp.where(inner, z_in[q, 1, j, at[p]].astype(f32), 0.0)

    def swap(l, s):
        q = 2 * l + s
        if REDUCE[l][s] == "x":
            for p in range(PIECES):
                cross[q, 0, 1, at[p]] = gathered(q, 1, p, pair_sum(q, 0, 1, p)).astype(bf16)
                rx_go(q, 0, p)

    def finish(l, s):
        q = 2 * l + s
        for p in range(PIECES):
            value = gathered(q, 0, p, pair_sum(q, 0, 0, p))
            if REDUCE[l][s] == "x":
                rx_wait(q, 0, p)
            value = value + x_in[q, 0, at[p]].astype(f32)
            here = pl.ds(s * size + p * cut, cut)
            if l == 0:
                now = (tokens[here].astype(f32) + value).astype(bf16)
                mixed[here] = now
                wide = now.astype(f32)
                inv_rms = lax.rsqrt(jnp.mean(wide * wide, axis=1, keepdims=True) + 1e-06)
                rows2[s, z, 0, at[p]] = (wide * inv_rms * gain_ref[...]).astype(bf16)
            else:
                out[here] = (mixed[here].astype(f32) + value).astype(bf16)
        if l == 0:
            start(1, s)

    steps = {
        "S": start, "W": weights, "a": functools.partial(arrive, 0),
        "b": functools.partial(arrive, 1), "x": x_arrive, "C": compute, "k": core_arrive, "t": functools.partial(total, 0), "u": functools.partial(total, 1), "f": swap,
        "F": finish,
    }
    for word in " ".join(PROGRAM).split():
        steps[word[0]](*[int(c) for c in word[1:]])
    for copy, when in sends:
        if when is None:
            copy.wait_send()
        else:
            pl.when(when)(copy.wait_send)


def fused_shards(
    tokens, experts_one, gates_one, w_in_one, w_down_one, norm_gain,
    experts_two, gates_two, placement_two, w_in_two, w_down_two,
):
    experts = placement_two.shape[0]
    tok, width = tokens.shape
    half = w_down_one.shape[1]
    n = lax.axis_size("ep")
    bf16 = jnp.bfloat16
    dma = pltpu.SemaphoreType.DMA
    size = tok // STREAMS
    q = 2 * STREAMS
    vmem = pl.BlockSpec(memory_space=pltpu.VMEM)
    hbm = pl.BlockSpec(memory_space=pl.ANY)
    top = experts_one.shape[1]
    return pl.pallas_call(
        functools.partial(fused_kernel, n, experts, width),
        out_shape=jax.ShapeDtypeStruct((tok, width), bf16),
        in_specs=[hbm] * 5 + [vmem, pl.BlockSpec(memory_space=pltpu.SMEM)] + [hbm] * 4,
        out_specs=vmem,
        scratch_shapes=[
            pltpu.VMEM((tok, width), bf16),
            pltpu.VMEM((2, top, tok), jnp.int32),
            pltpu.VMEM((2, top, tok), jnp.float32),
            pltpu.VMEM((tok, width), bf16),
            pltpu.VMEM((STREAMS, n, 4, size, width + LANES), bf16),
            pltpu.VMEM((STREAMS, n, 4, size, width), bf16),
            pltpu.VMEM((q, n, 4, size, width), bf16),
            pltpu.VMEM((q, n, 2, size, width), bf16),
            pltpu.VMEM((q, n, 2, size, width), bf16),
            pltpu.VMEM((q, n, size, width), bf16),
            pltpu.VMEM((q, 5, 2, size, width), bf16),
            pltpu.VMEM((width, 2, half), bf16),
            pltpu.VMEM((2, width, 2 * half), bf16),
            pltpu.VMEM((2, half, width), bf16),
            pltpu.VMEM((4 * size, half), bf16),
            dma((9,)),
            dma((q, 5, 2, PIECES)),
            dma((q, n, 2, PIECES)),
            dma((q, n, PIECES)),
            dma((q, n, PIECES)),
            dma((q, n, 2)),
            dma((q, n, 2)),
            dma((q, n)),
            dma((q, n)),
            dma((q, n, PIECES)),
            dma((q, n, PIECES)),
            dma((q, n, 2, PIECES)),
            dma((q, 5, 2, PIECES)),
        ],
        compiler_params=pltpu.CompilerParams(
            collective_id=0, has_side_effects=True, vmem_limit_bytes=63 * 1000 * 1000
        ),
        name="layers",
    )(
        tokens, experts_one.T, gates_one.T, experts_two.T, gates_two.T, norm_gain.reshape(1, width), placement_two,
        w_in_one.reshape(width, 2, half), w_down_one.reshape(half, width),
        w_in_two.reshape(width, 2, half), w_down_two.reshape(half, width),
    )


def capacity(tok_rows, top_count, expert_count):
    return max(2, min(tok_rows, 5 * tok_rows * top_count // (4 * expert_count)))


def pack_rows(rows_in, targets, expert_count, per_slot):
    tok_rows, top_count = targets.shape
    flat_ids = targets.reshape(-1)
    hit_table = (flat_ids[:, None] == jnp.arange(expert_count, dtype=jnp.int32)[None, :]).astype(
        jnp.int32
    )
    before = jnp.cumsum(hit_table, axis=0) - hit_table
    slot_rank = jnp.sum(before * hit_table, axis=1)
    slot_index = flat_ids * per_slot + slot_rank
    source = jnp.arange(tok_rows * top_count, dtype=jnp.int32) // top_count
    owner_row = jnp.zeros((expert_count * per_slot,), jnp.int32).at[slot_index].set(source)
    filled = jnp.zeros((expert_count * per_slot,), jnp.int32).at[slot_index].set(1)
    buffer = jnp.where(filled[:, None] > 0, rows_in[owner_row], jnp.zeros((), rows_in.dtype))
    return (buffer, slot_index)


def to_experts(buffer, expert_count, per_slot):
    row_width = buffer.shape[1]
    arrived = lax.all_to_all(
        buffer.reshape(expert_count, per_slot, row_width),
        ("ep", "dp"),
        split_axis=0,
        concat_axis=0,
        tiled=True,
    )
    return arrived.reshape(expert_count * per_slot, row_width)


def to_owners(produced, expert_count, per_slot):
    row_width = produced.shape[1]
    returned = lax.all_to_all(
        produced.reshape(expert_count, per_slot, row_width),
        ("ep", "dp"),
        split_axis=0,
        concat_axis=0,
        tiled=True,
    )
    return returned.reshape(expert_count * per_slot, row_width)


def run_expert(received, w_in, w_down):
    row_width = received.shape[1]
    down_local = w_down[0]
    half_width = down_local.shape[0]
    w_local = w_in.reshape(row_width, 2 * half_width)
    gate_up = jnp.dot(
        lax.all_gather(received, "tp", axis=0, tiled=True),
        w_local,
        preferred_element_type=jnp.float32,
    )
    hidden = (jax.nn.silu(gate_up[:, :half_width]) * gate_up[:, half_width:]).astype(jnp.bfloat16)
    return lax.psum_scatter(
        jnp.dot(hidden, down_local, preferred_element_type=jnp.float32).astype(jnp.bfloat16),
        "tp",
        scatter_dimension=0,
        tiled=True,
    )


def moe_block(rows_in, targets, gate_values, w_in, w_down, expert_count, per_slot):
    tok_rows, top_count = targets.shape
    row_width = rows_in.shape[1]
    buffer, slot_index = pack_rows(rows_in, targets, expert_count, per_slot)
    arrived = to_experts(buffer, expert_count, per_slot)
    produced = run_expert(arrived, w_in, w_down)
    returned = to_owners(produced, expert_count, per_slot)
    picked = returned[slot_index].reshape(tok_rows, top_count, row_width)
    return jnp.sum(gate_values[:, :, None] * picked.astype(jnp.float32), axis=1)


def shards(
    tokens,
    experts_one,
    gates_one,
    w_in_one,
    w_down_one,
    norm_gain,
    experts_two,
    gates_two,
    placement_two,
    w_in_two,
    w_down_two,
):
    tok_rows, top_count = experts_one.shape
    expert_count = placement_two.shape[0]
    per_slot = capacity(tok_rows, top_count, expert_count)
    moe_one = moe_block(
        tokens, experts_one, gates_one, w_in_one, w_down_one, expert_count, per_slot
    )
    mixed = (tokens.astype(jnp.float32) + moe_one).astype(jnp.bfloat16)
    mixed = lax.optimization_barrier(mixed)
    mixed_wide = mixed.astype(jnp.float32)
    inv_rms = lax.rsqrt(jnp.mean(mixed_wide * mixed_wide, axis=1, keepdims=True) + 1e-06)
    normed = (mixed_wide * inv_rms * norm_gain[None, :]).astype(jnp.bfloat16)
    expert_range = jnp.arange(expert_count, dtype=jnp.int32)
    matches = experts_two[:, :, None] == expert_range[None, None, :]
    layer_slots = jnp.sum(jnp.where(matches, placement_two[None, None, :], 0), axis=2)
    moe_two = moe_block(
        normed, layer_slots, gates_two, w_in_two, w_down_two, expert_count, per_slot
    )
    return (mixed_wide + moe_two).astype(jnp.bfloat16)


def solution(mesh):
    in_specs = (
        P(("groups", "ep", "dp", "tp"), None),
        P(("groups", "ep", "dp", "tp"), None),
        P(("groups", "ep", "dp", "tp"), None),
        P(("ep", "dp"), None, None, "tp"),
        P(("ep", "dp"), "tp", None),
        P(),
        P(("groups", "ep", "dp", "tp"), None),
        P(("groups", "ep", "dp", "tp"), None),
        P(),
        P(("ep", "dp"), None, None, "tp"),
        P(("ep", "dp"), "tp", None),
    )
    out_specs = P(("groups", "ep", "dp", "tp"), None)
    ready = mesh.shape["tp"] == 1 and mesh.shape["dp"] == 4 and mesh.shape["ep"] == 4

    def body(*arrays):
        return (fused_shards if ready and arrays[0].shape[0] % 32 == 0 else shards)(*arrays)

    return jax.shard_map(body, mesh=mesh, in_specs=in_specs, out_specs=out_specs, check_vma=False)
```

```python
import functools

import jax
import jax.numpy as jnp
from jax import lax
from jax.experimental import pallas as pl
from jax.experimental.pallas import tpu as pltpu
from jax.sharding import PartitionSpec as P

MESH = pl.DeviceIdType.MESH
LANES = 128


STREAMS = 2
PIECES = 2
GATHER = ("zx", "zx")
REDUCE = ("zz", "xz")
OUTER = (
    "S00 S01 x000 W0",
    "a002 x010 a001 C000",
    "C010 x002 a003 C002",
    "k000 x003 a011 k002",
    "x001 C003 b011 C001",
    "k003 t002 C011 b013",
    "k001 k010 t000 a013",
    "t003 a012 C013 t001",
    "b012 k013 k011 C012",
    "t013 t010 k012 F00",
    "t012 a101 W1 t011",
    "a102 x100 F01 x101",
    "a103 x102 C101 x110",
    "C102 x103 k102 t102",
    "C103 u102 C100 C110",
    "k103 b111 k101 a111",
    "u103 a113 k110 t103",
    "b113 t101 a112 C113",
    "b112 C111 k100 k113",
    "t110 u101 C112 t113",
    "k112 k111 t112 f10",
    "t111 F10 F11",
)
INNER = (
    "S00 a002 a001 x000",
    "S01 W0 C000 x002",
    "a003 a012 b011 x001",
    "a011 C002 x010 k000",
    "k002 x003 b013 C011",
    "C003 a013 k011 C001",
    "k003 C010 b012 C013",
    "t002 k001 k010 t003",
    "k013 C012 t001 k012",
    "t010 t000 F00 t013",
    "a102 a101 t011 x100",
    "t012 a103 F01 W1",
    "a111 a112 x110 x103",
    "x101 x102 a113 b111",
    "C101 C102 b113 b112",
    "C103 k101 C113 k102",
    "t102 k103 C111 u103",
    "C110 k113 t103 C100",
    "k110 k111 C112 u102",
    "t101 u101 t113 t110",
    "k100 k112 f10 t111",
    "t112 F10 F11",
)


def segments(lines):
    parts, calls = [[]], []
    for word in " ".join(lines).split():
        if word[0] == "C":
            calls.append([int(c) for c in word[1:]])
            parts.append([])
        else:
            parts[-1].append(word)
    return parts, calls


def fused_kernel(
    n, experts, width, tokens_hbm, experts_hbm, gates_hbm, experts2_hbm, gates2_hbm, gain_ref, place, w_in1, w_down1,
    w_in2, w_down2, out, tokens, ids, gates, mixed, rows1, rows2, part, core_in, cross, x_in, z_in, raw, w_in, w_down,
    hidden, gate_up, w_sem, z_send, z_recv, x_send, x_recv, c_send, c_recv, rc_send, rc_recv, rx_send, rx_recv, rz_send, rz_recv,
):
    z = lax.axis_index("ep")
    d = lax.axis_index("dp")
    mine = z * lax.axis_size("dp") + d
    x_peer = {"dp": (d + 2) % 4}
    c_peer = {"dp": d + 1 - 2 * (d % 2)}
    half = w_down.shape[1]
    tok = tokens.shape[0]
    size = tok // STREAMS
    pair = z + 1 - 2 * (z % 2)
    other = 3 - z
    order = [z, pair, 2 - z // 2, 3 - 3 * (z // 2)]
    inner = z % 3 != 0
    outer = jnp.logical_not(inner)
    rows = [rows1, rows2]
    f32, bf16 = jnp.float32, jnp.bfloat16
    cut = size // PIECES
    at = [pl.ds(p * cut, cut) for p in range(PIECES)]

    def remote(src, dst, send, recv, to):
        return pltpu.make_async_remote_copy(
            src_ref=src, dst_ref=dst, send_sem=send, recv_sem=recv, device_id=to, device_id_type=MESH
        )

    small = [
        pltpu.make_async_copy(src, dst, w_sem.at[k])
        for k, (src, dst) in enumerate(
            [
                (tokens_hbm, tokens), (experts_hbm, ids.at[0]), (gates_hbm, gates.at[0]),
                (experts2_hbm, ids.at[1]), (gates2_hbm, gates.at[1]),
            ]
        )
    ]
    load_in = [pltpu.make_async_copy(w, raw, w_sem.at[5 + k]) for k, w in enumerate((w_in1, w_in2))]
    load_down = [pltpu.make_async_copy(w, w_down.at[k], w_sem.at[7 + k]) for k, w in enumerate((w_down1, w_down2))]
    for copy in small + [load_in[0], load_down[0], load_down[1]]:
        copy.start()

    barrier = pltpu.get_barrier_semaphore()
    pl.semaphore_signal(barrier, inc=1, device_id={"ep": pair}, device_id_type=MESH)
    pl.semaphore_signal(barrier, inc=1, device_id=x_peer, device_id_type=MESH)
    pl.semaphore_signal(barrier, inc=1, device_id=c_peer, device_id_type=MESH)

    @pl.when(inner)
    def _():
        pl.semaphore_signal(barrier, inc=1, device_id={"ep": other}, device_id_type=MESH)

    common = []
    sends = {False: [], True: []}

    def go(make, ins=None):
        make().start()
        (common if ins is None else sends[ins]).append(make)

    for copy in small:
        copy.wait()
    lane = lax.broadcasted_iota(jnp.int32, (LANES, tok), 0)
    table = jnp.zeros((LANES, tok), f32)
    for l in range(2):
        here = jnp.where(lane // (2 * experts) == l, lane % experts, -1)
        for k in range(ids.shape[1]):
            table += jnp.where(ids[l, k : k + 1] == here, gates[l, k : k + 1], 0.0)
    high = table.astype(bf16).astype(f32)
    table = jnp.where((lane // experts) % 2 == 0, high, table - high).T.astype(bf16)
    for s in range(STREAMS):
        own = pl.ds(s * size, size)
        rows1[s, z, 0, :, :width] = tokens[own]
        rows1[s, z, 0, :, width:] = table[s * size : (s + 1) * size]
    e_mine = 0
    for e in range(experts):
        e_mine = e_mine + jnp.where(place[e] == mine, e, 0)
    lanes = [mine, 2 * experts + e_mine]

    @pl.when(inner)
    def _():
        pl.semaphore_wait(barrier, 4)

    @pl.when(outer)
    def _():
        pl.semaphore_wait(barrier, 3)

    def block(l, s, b, j):
        return rows[l].at[s, b, j]

    def z_move(l, s, b, j, p, k, to):
        q = 2 * l + s
        spot = block(l, s, b, j).at[at[p]]
        return remote(spot, spot, z_send.at[q, k, j, p], z_recv.at[q, b, j, p], {"ep": to})

    def z_own(ins, l, s, j):
        for p in range(PIECES):
            go(functools.partial(z_move, l, s, z, j, p, 0, pair), ins)
            if ins:
                go(functools.partial(z_move, l, s, z, j, p, 1, other), ins)

    def x_move(ins, l, s, i, p):
        q, b = 2 * l + s, order[i]

        def make():
            spot, there = block(l, s, b, 0).at[at[p]], block(l, s, b, 1).at[at[p]]
            return remote(spot, there, x_send.at[q, i, p], x_recv.at[q, i, p], x_peer)

        go(make, ins)

    def c_move(ins, l, s, i, j):
        q, b = 2 * l + s, order[i]

        def make():
            return remote(block(l, s, b, j), block(l, s, b, 2 + j), c_send.at[q, i, j], c_recv.at[q, i, j], c_peer)

        go(make, ins)

    def start(ins, l, s):
        z_own(ins, l, s, 0)
        for p in range(PIECES):
            x_move(ins, l, s, 0, p)
        c_move(ins, l, s, 0, 0)

    def arrive(j, ins, l, s, i):
        for p in range(PIECES):
            move = functools.partial(z_move, l, s, order[i], j, p, 1 + i, other if i == 1 else pair)
            move().wait_recv()
            if ins:
                go(move, ins)
            if GATHER[l][s] == "z":
                x_move(ins, l, s, i, p)
        c_move(ins, l, s, i, j)

    def x_arrive(ins, l, s, i):
        q, b = 2 * l + s, order[i]
        for p in range(PIECES):
            spot = block(l, s, b, 1).at[at[p]]
            remote(spot, spot, x_send.at[q, i, p], x_recv.at[q, i, p], x_peer).wait_recv()
        if GATHER[l][s] == "x":
            z_own(ins, l, s, 1)
        c_move(ins, l, s, i, 1)

    def weights(ins, l):
        load_in[l].wait()
        group = 128

        @pl.loop(0, width // group)
        def _(j):
            here = pl.ds(pl.multiple_of(j * group, group), group)
            w_in[l, here] = raw[here].reshape(group, 2 * half)

        load_down[l].wait()
        if l == 0:
            load_in[1].start()

    def pick(a, b):
        return a if a is b or isinstance(a, int) and isinstance(b, int) and a == b else jnp.where(inner, b, a)

    def compute(l, outer_at, inner_at):
        s = pick(outer_at[0], inner_at[0])
        i = pick(outer_at[1], inner_at[1])
        b = pick(order[outer_at[1]], order[inner_at[1]])
        q = 2 * l + s
        for j in range(2):
            spot = block(l, s, b, 2 + j)
            remote(spot, spot, c_send.at[q, i, j], c_recv.at[q, i, j], c_peer).wait_recv()
        count = 4 * size
        marks = rows1[s, b, :, :, width:].reshape(count, LANES).astype(f32)
        spots = lax.broadcasted_iota(jnp.int32, (count, LANES), 1)
        hit = (spots == lanes[l]) | (spots == lanes[l] + experts)
        weight = jnp.sum(jnp.where(hit, marks, 0.0), axis=1, keepdims=True)

        @pl.loop(0, 2)
        def _(j):
            x = rows[l][s, b, :, :, :width].reshape(count, width)
            here = pl.multiple_of(j * half, LANES)
            gate_up[j] = jnp.dot(x, w_in[l, :, pl.ds(here, half)], preferred_element_type=f32)

        gate = gate_up[0]
        hidden[...] = (gate / (1.0 + jnp.exp(-gate)) * gate_up[1]).astype(bf16)
        y = jnp.dot(hidden[...], w_down[l], preferred_element_type=f32)
        y = jnp.where(weight == 0.0, 0.0, y * weight)
        part[q, i] = y.astype(bf16).reshape(4, size, width)

        def make():
            return remote(part.at[q, i, pl.ds(2, 2)], core_in.at[q, i], rc_send.at[q, i], rc_recv.at[q, i], c_peer)

        go(make)

    def pair_sum(q, i, j, p):
        return part[q, i, j, at[p]].astype(f32) + core_in[q, i, j, at[p]].astype(f32)

    def z_wait(q, slot, j, p):
        spot = z_in.at[q, slot, j, at[p]]
        remote(spot, spot, rz_send.at[q, 0, j, p], rz_recv.at[q, slot, j, p], {"ep": pair}).wait_recv()

    def line(ins, q, i, j, p, value):
        if ins:
            slot_in = {1: 4, 2: 2, 3: 3}[i]
            z_wait(q, slot_in, j, p)
            value = value + z_in[q, slot_in, j, at[p]].astype(f32)
        slot = {1: 0, 2: 1, 3: 4}[i] if ins else {1: 0, 2: 2, 3: 3}[i]
        to = other if ins and i > 1 else pair
        cross[q, i, j, at[p]] = value.astype(bf16)

        def make():
            spot, there = cross.at[q, i, j, at[p]], z_in.at[q, slot, j, at[p]]
            return remote(spot, there, rz_send.at[q, i, j, p], rz_recv.at[q, slot, j, p], {"ep": to})

        go(make, ins)

    def rx_go(ins, q, i, p):
        def make():
            spot, there = cross.at[q, i, 1, at[p]], x_in.at[q, i, at[p]]
            return remote(spot, there, rx_send.at[q, i, p], rx_recv.at[q, i, p], x_peer)

        go(make, ins)

    def rx_wait(q, i, p):
        spot = x_in.at[q, i, at[p]]
        remote(spot, spot, rx_send.at[q, i, p], rx_recv.at[q, i, p], x_peer).wait_recv()

    def core_arrive(ins, l, s, i):
        q = 2 * l + s
        remote(core_in.at[q, i], core_in.at[q, i], rc_send.at[q, i], rc_recv.at[q, i], c_peer).wait_recv()
        if REDUCE[l][s] == "z":
            for p in range(PIECES):
                cross[q, i, 1, at[p]] = pair_sum(q, i, 1, p).astype(bf16)
                rx_go(ins, q, i, p)

    def total(j, ins, l, s, i):
        q = 2 * l + s
        for p in range(PIECES):
            if REDUCE[l][s] == "z":
                rx_wait(q, i, p)
            if i > 0:
                value = pair_sum(q, i, j, p)
                if REDUCE[l][s] == "z":
                    value = value + x_in[q, i, at[p]].astype(f32)
                line(ins, q, i, j, p, value)

    def gathered(ins, q, j, p):
        value = pair_sum(q, 0, j, p)
        for slot in range(2 if ins else 1):
            z_wait(q, slot, j, p)
            value = value + z_in[q, slot, j, at[p]].astype(f32)
        return value

    def swap(ins, l, s):
        q = 2 * l + s
        for p in range(PIECES):
            cross[q, 0, 1, at[p]] = gathered(ins, q, 1, p).astype(bf16)
            rx_go(ins, q, 0, p)

    def finish(ins, l, s):
        q = 2 * l + s
        for p in range(PIECES):
            value = gathered(ins, q, 0, p)
            if REDUCE[l][s] == "x":
                rx_wait(q, 0, p)
            value = value + x_in[q, 0, at[p]].astype(f32)
            here = pl.ds(s * size + p * cut, cut)
            if l == 0:
                now = (tokens[here].astype(f32) + value).astype(bf16)
                mixed[here] = now
                wide = now.astype(f32)
                inv_rms = lax.rsqrt(jnp.mean(wide * wide, axis=1, keepdims=True) + 1e-06)
                rows2[s, z, 0, at[p]] = (wide * inv_rms * gain_ref[...]).astype(bf16)
            else:
                out[here] = (mixed[here].astype(f32) + value).astype(bf16)
        if l == 0:
            start(ins, 1, s)

    steps = {
        "S": start, "W": weights, "x": x_arrive, "k": core_arrive, "f": swap, "F": finish,
        "a": functools.partial(arrive, 0), "b": functools.partial(arrive, 1),
        "t": functools.partial(total, 0), "u": functools.partial(total, 1),
    }

    def run(ins, words):
        for word in words:
            steps[word[0]](ins, *[int(c) for c in word[1:]])

    plans = {False: segments(OUTER), True: segments(INNER)}
    for k in range(len(plans[True][0])):
        for ins, when in ((False, outer), (True, inner)):
            if plans[ins][0][k]:
                pl.when(when)(functools.partial(run, ins, plans[ins][0][k]))
        if k < len(plans[True][1]):
            (l, *outer_at), (_, *inner_at) = plans[False][1][k], plans[True][1][k]
            compute(l, outer_at, inner_at)
    for make in common:
        make().wait_send()
    for ins, when in ((False, outer), (True, inner)):

        @pl.when(when)
        def _(ins=ins):
            for make in sends[ins]:
                make().wait_send()


def fused_shards(
    tokens, experts_one, gates_one, w_in_one, w_down_one, norm_gain,
    experts_two, gates_two, placement_two, w_in_two, w_down_two,
):
    experts = placement_two.shape[0]
    tok, width = tokens.shape
    half = w_down_one.shape[1]
    n = lax.axis_size("ep")
    bf16 = jnp.bfloat16
    dma = pltpu.SemaphoreType.DMA
    size = tok // STREAMS
    q = 2 * STREAMS
    vmem = pl.BlockSpec(memory_space=pltpu.VMEM)
    hbm = pl.BlockSpec(memory_space=pl.ANY)
    top = experts_one.shape[1]
    return pl.pallas_call(
        functools.partial(fused_kernel, n, experts, width),
        out_shape=jax.ShapeDtypeStruct((tok, width), bf16),
        in_specs=[hbm] * 5 + [vmem, pl.BlockSpec(memory_space=pltpu.SMEM)] + [hbm] * 4,
        out_specs=vmem,
        scratch_shapes=[
            pltpu.VMEM((tok, width), bf16),
            pltpu.VMEM((2, top, tok), jnp.int32),
            pltpu.VMEM((2, top, tok), jnp.float32),
            pltpu.VMEM((tok, width), bf16),
            pltpu.VMEM((STREAMS, n, 4, size, width + LANES), bf16),
            pltpu.VMEM((STREAMS, n, 4, size, width), bf16),
            pltpu.VMEM((q, n, 4, size, width), bf16),
            pltpu.VMEM((q, n, 2, size, width), bf16),
            pltpu.VMEM((q, n, 2, size, width), bf16),
            pltpu.VMEM((q, n, size, width), bf16),
            pltpu.VMEM((q, 5, 2, size, width), bf16),
            pltpu.VMEM((width, 2, half), bf16),
            pltpu.VMEM((2, width, 2 * half), bf16),
            pltpu.VMEM((2, half, width), bf16),
            pltpu.VMEM((4 * size, half), bf16),
            pltpu.VMEM((2, 4 * size, half), jnp.float32),
            dma((9,)),
            dma((q, 5, 2, PIECES)),
            dma((q, n, 2, PIECES)),
            dma((q, n, PIECES)),
            dma((q, n, PIECES)),
            dma((q, n, 2)),
            dma((q, n, 2)),
            dma((q, n)),
            dma((q, n)),
            dma((q, n, PIECES)),
            dma((q, n, PIECES)),
            dma((q, n, 2, PIECES)),
            dma((q, 5, 2, PIECES)),
        ],
        compiler_params=pltpu.CompilerParams(
            collective_id=0, has_side_effects=True, vmem_limit_bytes=63 * 1000 * 1000
        ),
        name="layers",
    )(
        tokens, experts_one.T, gates_one.T, experts_two.T, gates_two.T, norm_gain.reshape(1, width), placement_two,
        w_in_one.reshape(width, 2, half), w_down_one.reshape(half, width),
        w_in_two.reshape(width, 2, half), w_down_two.reshape(half, width),
    )


def capacity(tok_rows, top_count, expert_count):
    return max(2, min(tok_rows, 5 * tok_rows * top_count // (4 * expert_count)))


def pack_rows(rows_in, targets, expert_count, per_slot):
    tok_rows, top_count = targets.shape
    flat_ids = targets.reshape(-1)
    hit_table = (flat_ids[:, None] == jnp.arange(expert_count, dtype=jnp.int32)[None, :]).astype(
        jnp.int32
    )
    before = jnp.cumsum(hit_table, axis=0) - hit_table
    slot_rank = jnp.sum(before * hit_table, axis=1)
    slot_index = flat_ids * per_slot + slot_rank
    source = jnp.arange(tok_rows * top_count, dtype=jnp.int32) // top_count
    owner_row = jnp.zeros((expert_count * per_slot,), jnp.int32).at[slot_index].set(source)
    filled = jnp.zeros((expert_count * per_slot,), jnp.int32).at[slot_index].set(1)
    buffer = jnp.where(filled[:, None] > 0, rows_in[owner_row], jnp.zeros((), rows_in.dtype))
    return (buffer, slot_index)


def to_experts(buffer, expert_count, per_slot):
    row_width = buffer.shape[1]
    arrived = lax.all_to_all(
        buffer.reshape(expert_count, per_slot, row_width),
        ("ep", "dp"),
        split_axis=0,
        concat_axis=0,
        tiled=True,
    )
    return arrived.reshape(expert_count * per_slot, row_width)


def to_owners(produced, expert_count, per_slot):
    row_width = produced.shape[1]
    returned = lax.all_to_all(
        produced.reshape(expert_count, per_slot, row_width),
        ("ep", "dp"),
        split_axis=0,
        concat_axis=0,
        tiled=True,
    )
    return returned.reshape(expert_count * per_slot, row_width)


def run_expert(received, w_in, w_down):
    row_width = received.shape[1]
    down_local = w_down[0]
    half_width = down_local.shape[0]
    w_local = w_in.reshape(row_width, 2 * half_width)
    gate_up = jnp.dot(
        lax.all_gather(received, "tp", axis=0, tiled=True),
        w_local,
        preferred_element_type=jnp.float32,
    )
    hidden = (jax.nn.silu(gate_up[:, :half_width]) * gate_up[:, half_width:]).astype(jnp.bfloat16)
    return lax.psum_scatter(
        jnp.dot(hidden, down_local, preferred_element_type=jnp.float32).astype(jnp.bfloat16),
        "tp",
        scatter_dimension=0,
        tiled=True,
    )


def moe_block(rows_in, targets, gate_values, w_in, w_down, expert_count, per_slot):
    tok_rows, top_count = targets.shape
    row_width = rows_in.shape[1]
    buffer, slot_index = pack_rows(rows_in, targets, expert_count, per_slot)
    arrived = to_experts(buffer, expert_count, per_slot)
    produced = run_expert(arrived, w_in, w_down)
    returned = to_owners(produced, expert_count, per_slot)
    picked = returned[slot_index].reshape(tok_rows, top_count, row_width)
    return jnp.sum(gate_values[:, :, None] * picked.astype(jnp.float32), axis=1)


def shards(
    tokens,
    experts_one,
    gates_one,
    w_in_one,
    w_down_one,
    norm_gain,
    experts_two,
    gates_two,
    placement_two,
    w_in_two,
    w_down_two,
):
    tok_rows, top_count = experts_one.shape
    expert_count = placement_two.shape[0]
    per_slot = capacity(tok_rows, top_count, expert_count)
    moe_one = moe_block(
        tokens, experts_one, gates_one, w_in_one, w_down_one, expert_count, per_slot
    )
    mixed = (tokens.astype(jnp.float32) + moe_one).astype(jnp.bfloat16)
    mixed = lax.optimization_barrier(mixed)
    mixed_wide = mixed.astype(jnp.float32)
    inv_rms = lax.rsqrt(jnp.mean(mixed_wide * mixed_wide, axis=1, keepdims=True) + 1e-06)
    normed = (mixed_wide * inv_rms * norm_gain[None, :]).astype(jnp.bfloat16)
    expert_range = jnp.arange(expert_count, dtype=jnp.int32)
    matches = experts_two[:, :, None] == expert_range[None, None, :]
    layer_slots = jnp.sum(jnp.where(matches, placement_two[None, None, :], 0), axis=2)
    moe_two = moe_block(
        normed, layer_slots, gates_two, w_in_two, w_down_two, expert_count, per_slot
    )
    return (mixed_wide + moe_two).astype(jnp.bfloat16)


def solution(mesh):
    in_specs = (
        P(("groups", "ep", "dp", "tp"), None),
        P(("groups", "ep", "dp", "tp"), None),
        P(("groups", "ep", "dp", "tp"), None),
        P(("ep", "dp"), None, None, "tp"),
        P(("ep", "dp"), "tp", None),
        P(),
        P(("groups", "ep", "dp", "tp"), None),
        P(("groups", "ep", "dp", "tp"), None),
        P(),
        P(("ep", "dp"), None, None, "tp"),
        P(("ep", "dp"), "tp", None),
    )
    out_specs = P(("groups", "ep", "dp", "tp"), None)
    ready = mesh.shape["tp"] == 1 and mesh.shape["dp"] == 4 and mesh.shape["ep"] == 4

    def body(*arrays):
        return (fused_shards if ready and arrays[0].shape[0] % 32 == 0 else shards)(*arrays)

    return jax.shard_map(body, mesh=mesh, in_specs=in_specs, out_specs=out_specs, check_vma=False)
```

```python
import functools

import jax
import jax.numpy as jnp
from jax import lax
from jax.experimental import pallas as pl
from jax.experimental.pallas import tpu as pltpu
from jax.sharding import PartitionSpec as P

MESH = pl.DeviceIdType.MESH
LANES = 128


STREAMS = 2
PIECES = 2
GATHER = ("zx", "zx")
REDUCE = ("zz", "xz")
OUTER = (
    "S00 S01 a001 W0",
    "x010 a002 x001 x000",
    "C010 a003 x002 C001",
    "C002 k001 x003 C000",
    "k002 C003 a013 a011",
    "b013 b011 k003 k000",
    "t002 C013 t003 t001",
    "k013 C011 a012 b012",
    "k011 t013 t000 k010",
    "C012 k012 F00 t012",
    "t011 t010 a101 W1",
    "F01 x101 x110 a103",
    "C101 x100 C110 k101",
    "a102 u101 t101 x103",
    "C100 C103 k110 x102",
    "k103 u103 a113 a111",
    "C102 t110 b113 t103",
    "k102 u102 a112 t102",
    "C113 k113 b112 k100",
    "b111 C112 t113 k112",
    "C111 k111 t112 f10",
    "t111 F11 F10",
)
INNER = (
    "S00 W0 S01 a002",
    "a001 a011 x000 a003",
    "C000 a013 b011 x002",
    "x010 x001 k000 C002",
    "b013 x003 C010 k002",
    "C001 k010 b012 C003",
    "a012 C013 k003 C011",
    "k001 t000 C012 k013",
    "t003 k011 k012 t002",
    "t001 t013 F00 W1",
    "t011 t010 a101 a102",
    "t012 a103 x101 F01",
    "C101 a111 x100 a112",
    "b111 x102 x103 a113",
    "b113 x110 C103 C110",
    "b112 C102 k103 u103",
    "k110 C113 C111 t103",
    "k102 C112 t110 k113",
    "u102 k101 C100 u101",
    "k111 t101 t113 t102",
    "k112 k100 t111 f10",
    "t112 F10 F11",
)


def segments(lines):
    parts, calls = [[]], []
    for word in " ".join(lines).split():
        if word[0] == "C":
            calls.append([int(c) for c in word[1:]])
            parts.append([])
        else:
            parts[-1].append(word)
    return parts, calls


def fused_kernel(
    n, experts, width, tokens_hbm, experts_hbm, gates_hbm, experts2_hbm, gates2_hbm, gain_ref, place, w_in1, w_down1,
    w_in2, w_down2, out, tokens, ids, gates, mixed, rows1, rows2, part, core_in, cross, x_in, z_in, raw, w_in, w_down,
    hidden, w_sem, z_send, z_recv, x_send, x_recv, c_send, c_recv, rc_send, rc_recv, rx_send, rx_recv, rz_send, rz_recv,
):
    z = lax.axis_index("ep")
    d = lax.axis_index("dp")
    mine = z * lax.axis_size("dp") + d
    x_peer = {"dp": (d + 2) % 4}
    c_peer = {"dp": d + 1 - 2 * (d % 2)}
    half = w_down.shape[1]
    tok = tokens.shape[0]
    size = tok // STREAMS
    pair = z + 1 - 2 * (z % 2)
    other = 3 - z
    order = [z, pair, 2 - z // 2, 3 - 3 * (z // 2)]
    inner = z % 3 != 0
    outer = jnp.logical_not(inner)
    rows = [rows1, rows2]
    f32, bf16 = jnp.float32, jnp.bfloat16
    cut = size // PIECES
    at = [pl.ds(p * cut, cut) for p in range(PIECES)]

    def remote(src, dst, send, recv, to):
        return pltpu.make_async_remote_copy(
            src_ref=src, dst_ref=dst, send_sem=send, recv_sem=recv, device_id=to, device_id_type=MESH
        )

    small = [
        pltpu.make_async_copy(src, dst, w_sem.at[k])
        for k, (src, dst) in enumerate(
            [
                (tokens_hbm, tokens), (experts_hbm, ids.at[0]), (gates_hbm, gates.at[0]),
                (experts2_hbm, ids.at[1]), (gates2_hbm, gates.at[1]),
            ]
        )
    ]
    load_in = [pltpu.make_async_copy(w, raw, w_sem.at[5 + k]) for k, w in enumerate((w_in1, w_in2))]
    load_down = [pltpu.make_async_copy(w, w_down.at[k], w_sem.at[7 + k]) for k, w in enumerate((w_down1, w_down2))]
    for copy in small + [load_in[0], load_down[0], load_down[1]]:
        copy.start()

    barrier = pltpu.get_barrier_semaphore()
    pl.semaphore_signal(barrier, inc=1, device_id={"ep": pair}, device_id_type=MESH)
    pl.semaphore_signal(barrier, inc=1, device_id=x_peer, device_id_type=MESH)
    pl.semaphore_signal(barrier, inc=1, device_id=c_peer, device_id_type=MESH)

    @pl.when(inner)
    def _():
        pl.semaphore_signal(barrier, inc=1, device_id={"ep": other}, device_id_type=MESH)

    common = []
    sends = {False: [], True: []}

    def go(make, ins=None):
        make().start()
        (common if ins is None else sends[ins]).append(make)

    for copy in small:
        copy.wait()
    lane = lax.broadcasted_iota(jnp.int32, (LANES, tok), 0)
    table = jnp.zeros((LANES, tok), f32)
    for l in range(2):
        here = jnp.where(lane // (2 * experts) == l, lane % experts, -1)
        for k in range(ids.shape[1]):
            table += jnp.where(ids[l, k : k + 1] == here, gates[l, k : k + 1], 0.0)
    high = table.astype(bf16).astype(f32)
    table = jnp.where((lane // experts) % 2 == 0, high, table - high).T.astype(bf16)
    for s in range(STREAMS):
        own = pl.ds(s * size, size)
        rows1[s, z, 0, :, :width] = tokens[own]
        rows1[s, z, 0, :, width:] = table[s * size : (s + 1) * size]
    e_mine = 0
    for e in range(experts):
        e_mine = e_mine + jnp.where(place[e] == mine, e, 0)
    lanes = [mine, 2 * experts + e_mine]

    @pl.when(inner)
    def _():
        pl.semaphore_wait(barrier, 4)

    @pl.when(outer)
    def _():
        pl.semaphore_wait(barrier, 3)

    def block(l, s, b, j):
        return rows[l].at[s, b, j]

    def z_move(l, s, b, j, p, k, to):
        q = 2 * l + s
        spot = block(l, s, b, j).at[at[p]]
        return remote(spot, spot, z_send.at[q, k, j, p], z_recv.at[q, b, j, p], {"ep": to})

    def z_own(ins, l, s, j):
        for p in range(PIECES):
            go(functools.partial(z_move, l, s, z, j, p, 0, pair), ins)
            if ins:
                go(functools.partial(z_move, l, s, z, j, p, 1, other), ins)

    def x_move(ins, l, s, i, p):
        q, b = 2 * l + s, order[i]

        def make():
            spot, there = block(l, s, b, 0).at[at[p]], block(l, s, b, 1).at[at[p]]
            return remote(spot, there, x_send.at[q, i, p], x_recv.at[q, i, p], x_peer)

        go(make, ins)

    def c_move(ins, l, s, i, j):
        q, b = 2 * l + s, order[i]

        def make():
            return remote(block(l, s, b, j), block(l, s, b, 2 + j), c_send.at[q, i, j], c_recv.at[q, i, j], c_peer)

        go(make, ins)

    def start(ins, l, s):
        z_own(ins, l, s, 0)
        for p in range(PIECES):
            x_move(ins, l, s, 0, p)
        c_move(ins, l, s, 0, 0)

    def arrive(j, ins, l, s, i):
        for p in range(PIECES):
            move = functools.partial(z_move, l, s, order[i], j, p, 1 + i, other if i == 1 else pair)
            move().wait_recv()
            if ins:
                go(move, ins)
            if GATHER[l][s] == "z":
                x_move(ins, l, s, i, p)
        c_move(ins, l, s, i, j)

    def x_arrive(ins, l, s, i):
        q, b = 2 * l + s, order[i]
        for p in range(PIECES):
            spot = block(l, s, b, 1).at[at[p]]
            remote(spot, spot, x_send.at[q, i, p], x_recv.at[q, i, p], x_peer).wait_recv()
        if GATHER[l][s] == "x":
            z_own(ins, l, s, 1)
        c_move(ins, l, s, i, 1)

    def weights(ins, l):
        load_in[l].wait()
        group = 128

        @pl.loop(0, width // group)
        def _(j):
            here = pl.ds(pl.multiple_of(j * group, group), group)
            w_in[l, here] = raw[here].reshape(group, 2 * half)

        load_down[l].wait()
        if l == 0:
            load_in[1].start()

    def pick(a, b):
        return a if a is b or isinstance(a, int) and isinstance(b, int) and a == b else jnp.where(inner, b, a)

    def compute(l, outer_at, inner_at):
        s = pick(outer_at[0], inner_at[0])
        i = pick(outer_at[1], inner_at[1])
        b = pick(order[outer_at[1]], order[inner_at[1]])
        q = 2 * l + s
        for j in range(2):
            spot = block(l, s, b, 2 + j)
            remote(spot, spot, c_send.at[q, i, j], c_recv.at[q, i, j], c_peer).wait_recv()
        count = 4 * size
        marks = rows1[s, b, :, :, width:].reshape(count, LANES).astype(f32)
        spots = lax.broadcasted_iota(jnp.int32, (count, LANES), 1)
        hit = (spots == lanes[l]) | (spots == lanes[l] + experts)
        weight = jnp.sum(jnp.where(hit, marks, 0.0), axis=1, keepdims=True)

        x = rows[l][s, b, :, :, :width].reshape(count, width)
        gate = jnp.dot(x, w_in[l, :, :half], preferred_element_type=f32)
        up = jnp.dot(x, w_in[l, :, half:], preferred_element_type=f32)
        hidden[...] = (gate / (1.0 + jnp.exp(-gate)) * up).astype(bf16)
        y = jnp.dot(hidden[...], w_down[l], preferred_element_type=f32)
        y = jnp.where(weight == 0.0, 0.0, y * weight)
        part[q, i] = y.astype(bf16).reshape(4, size, width)

        def make():
            return remote(part.at[q, i, pl.ds(2, 2)], core_in.at[q, i], rc_send.at[q, i], rc_recv.at[q, i], c_peer)

        go(make)

    def pair_sum(q, i, j, p):
        return part[q, i, j, at[p]].astype(f32) + core_in[q, i, j, at[p]].astype(f32)

    def z_wait(q, slot, j, p):
        spot = z_in.at[q, slot, j, at[p]]
        remote(spot, spot, rz_send.at[q, 0, j, p], rz_recv.at[q, slot, j, p], {"ep": pair}).wait_recv()

    def line(ins, q, i, j, p, value):
        if ins:
            slot_in = {1: 4, 2: 2, 3: 3}[i]
            z_wait(q, slot_in, j, p)
            value = value + z_in[q, slot_in, j, at[p]].astype(f32)
        slot = {1: 0, 2: 1, 3: 4}[i] if ins else {1: 0, 2: 2, 3: 3}[i]
        to = other if ins and i > 1 else pair
        cross[q, i, j, at[p]] = value.astype(bf16)

        def make():
            spot, there = cross.at[q, i, j, at[p]], z_in.at[q, slot, j, at[p]]
            return remote(spot, there, rz_send.at[q, i, j, p], rz_recv.at[q, slot, j, p], {"ep": to})

        go(make, ins)

    def rx_go(ins, q, i, p):
        def make():
            spot, there = cross.at[q, i, 1, at[p]], x_in.at[q, i, at[p]]
            return remote(spot, there, rx_send.at[q, i, p], rx_recv.at[q, i, p], x_peer)

        go(make, ins)

    def rx_wait(q, i, p):
        spot = x_in.at[q, i, at[p]]
        remote(spot, spot, rx_send.at[q, i, p], rx_recv.at[q, i, p], x_peer).wait_recv()

    def core_arrive(ins, l, s, i):
        q = 2 * l + s
        remote(core_in.at[q, i], core_in.at[q, i], rc_send.at[q, i], rc_recv.at[q, i], c_peer).wait_recv()
        if REDUCE[l][s] == "z":
            for p in range(PIECES):
                cross[q, i, 1, at[p]] = pair_sum(q, i, 1, p).astype(bf16)
                rx_go(ins, q, i, p)

    def total(j, ins, l, s, i):
        q = 2 * l + s
        for p in range(PIECES):
            if REDUCE[l][s] == "z":
                rx_wait(q, i, p)
            if i > 0:
                value = pair_sum(q, i, j, p)
                if REDUCE[l][s] == "z":
                    value = value + x_in[q, i, at[p]].astype(f32)
                line(ins, q, i, j, p, value)

    def gathered(ins, q, j, p):
        value = pair_sum(q, 0, j, p)
        for slot in range(2 if ins else 1):
            z_wait(q, slot, j, p)
            value = value + z_in[q, slot, j, at[p]].astype(f32)
        return value

    def swap(ins, l, s):
        q = 2 * l + s
        for p in range(PIECES):
            cross[q, 0, 1, at[p]] = gathered(ins, q, 1, p).astype(bf16)
            rx_go(ins, q, 0, p)

    def finish(ins, l, s):
        q = 2 * l + s
        for p in range(PIECES):
            value = gathered(ins, q, 0, p)
            if REDUCE[l][s] == "x":
                rx_wait(q, 0, p)
            value = value + x_in[q, 0, at[p]].astype(f32)
            here = pl.ds(s * size + p * cut, cut)
            if l == 0:
                now = (tokens[here].astype(f32) + value).astype(bf16)
                mixed[here] = now
                wide = now.astype(f32)
                inv_rms = lax.rsqrt(jnp.mean(wide * wide, axis=1, keepdims=True) + 1e-06)
                rows2[s, z, 0, at[p]] = (wide * inv_rms * gain_ref[...]).astype(bf16)
            else:
                out[here] = (mixed[here].astype(f32) + value).astype(bf16)
        if l == 0:
            start(ins, 1, s)

    steps = {
        "S": start, "W": weights, "x": x_arrive, "k": core_arrive, "f": swap, "F": finish,
        "a": functools.partial(arrive, 0), "b": functools.partial(arrive, 1),
        "t": functools.partial(total, 0), "u": functools.partial(total, 1),
    }

    def run(ins, words):
        for word in words:
            steps[word[0]](ins, *[int(c) for c in word[1:]])

    plans = {False: segments(OUTER), True: segments(INNER)}
    for k in range(len(plans[True][0])):
        for ins, when in ((False, outer), (True, inner)):
            if plans[ins][0][k]:
                pl.when(when)(functools.partial(run, ins, plans[ins][0][k]))
        if k < len(plans[True][1]):
            (l, *outer_at), (_, *inner_at) = plans[False][1][k], plans[True][1][k]
            compute(l, outer_at, inner_at)
    for make in common:
        make().wait_send()
    for ins, when in ((False, outer), (True, inner)):

        @pl.when(when)
        def _(ins=ins):
            for make in sends[ins]:
                make().wait_send()


def fused_shards(
    tokens, experts_one, gates_one, w_in_one, w_down_one, norm_gain,
    experts_two, gates_two, placement_two, w_in_two, w_down_two,
):
    experts = placement_two.shape[0]
    tok, width = tokens.shape
    half = w_down_one.shape[1]
    n = lax.axis_size("ep")
    bf16 = jnp.bfloat16
    dma = pltpu.SemaphoreType.DMA
    size = tok // STREAMS
    q = 2 * STREAMS
    vmem = pl.BlockSpec(memory_space=pltpu.VMEM)
    hbm = pl.BlockSpec(memory_space=pl.ANY)
    top = experts_one.shape[1]
    return pl.pallas_call(
        functools.partial(fused_kernel, n, experts, width),
        out_shape=jax.ShapeDtypeStruct((tok, width), bf16),
        in_specs=[hbm] * 5 + [vmem, pl.BlockSpec(memory_space=pltpu.SMEM)] + [hbm] * 4,
        out_specs=vmem,
        scratch_shapes=[
            pltpu.VMEM((tok, width), bf16),
            pltpu.VMEM((2, top, tok), jnp.int32),
            pltpu.VMEM((2, top, tok), jnp.float32),
            pltpu.VMEM((tok, width), bf16),
            pltpu.VMEM((STREAMS, n, 4, size, width + LANES), bf16),
            pltpu.VMEM((STREAMS, n, 4, size, width), bf16),
            pltpu.VMEM((q, n, 4, size, width), bf16),
            pltpu.VMEM((q, n, 2, size, width), bf16),
            pltpu.VMEM((q, n, 2, size, width), bf16),
            pltpu.VMEM((q, n, size, width), bf16),
            pltpu.VMEM((q, 5, 2, size, width), bf16),
            pltpu.VMEM((width, 2, half), bf16),
            pltpu.VMEM((2, width, 2 * half), bf16),
            pltpu.VMEM((2, half, width), bf16),
            pltpu.VMEM((4 * size, half), bf16),
            dma((9,)),
            dma((q, 5, 2, PIECES)),
            dma((q, n, 2, PIECES)),
            dma((q, n, PIECES)),
            dma((q, n, PIECES)),
            dma((q, n, 2)),
            dma((q, n, 2)),
            dma((q, n)),
            dma((q, n)),
            dma((q, n, PIECES)),
            dma((q, n, PIECES)),
            dma((q, n, 2, PIECES)),
            dma((q, 5, 2, PIECES)),
        ],
        compiler_params=pltpu.CompilerParams(
            collective_id=0, has_side_effects=True, vmem_limit_bytes=63 * 1000 * 1000
        ),
        name="layers",
    )(
        tokens, experts_one.T, gates_one.T, experts_two.T, gates_two.T, norm_gain.reshape(1, width), placement_two,
        w_in_one.reshape(width, 2, half), w_down_one.reshape(half, width),
        w_in_two.reshape(width, 2, half), w_down_two.reshape(half, width),
    )


def capacity(tok_rows, top_count, expert_count):
    return max(2, min(tok_rows, 5 * tok_rows * top_count // (4 * expert_count)))


def pack_rows(rows_in, targets, expert_count, per_slot):
    tok_rows, top_count = targets.shape
    flat_ids = targets.reshape(-1)
    hit_table = (flat_ids[:, None] == jnp.arange(expert_count, dtype=jnp.int32)[None, :]).astype(
        jnp.int32
    )
    before = jnp.cumsum(hit_table, axis=0) - hit_table
    slot_rank = jnp.sum(before * hit_table, axis=1)
    slot_index = flat_ids * per_slot + slot_rank
    source = jnp.arange(tok_rows * top_count, dtype=jnp.int32) // top_count
    owner_row = jnp.zeros((expert_count * per_slot,), jnp.int32).at[slot_index].set(source)
    filled = jnp.zeros((expert_count * per_slot,), jnp.int32).at[slot_index].set(1)
    buffer = jnp.where(filled[:, None] > 0, rows_in[owner_row], jnp.zeros((), rows_in.dtype))
    return (buffer, slot_index)


def to_experts(buffer, expert_count, per_slot):
    row_width = buffer.shape[1]
    arrived = lax.all_to_all(
        buffer.reshape(expert_count, per_slot, row_width),
        ("ep", "dp"),
        split_axis=0,
        concat_axis=0,
        tiled=True,
    )
    return arrived.reshape(expert_count * per_slot, row_width)


def to_owners(produced, expert_count, per_slot):
    row_width = produced.shape[1]
    returned = lax.all_to_all(
        produced.reshape(expert_count, per_slot, row_width),
        ("ep", "dp"),
        split_axis=0,
        concat_axis=0,
        tiled=True,
    )
    return returned.reshape(expert_count * per_slot, row_width)


def run_expert(received, w_in, w_down):
    row_width = received.shape[1]
    down_local = w_down[0]
    half_width = down_local.shape[0]
    w_local = w_in.reshape(row_width, 2 * half_width)
    gate_up = jnp.dot(
        lax.all_gather(received, "tp", axis=0, tiled=True),
        w_local,
        preferred_element_type=jnp.float32,
    )
    hidden = (jax.nn.silu(gate_up[:, :half_width]) * gate_up[:, half_width:]).astype(jnp.bfloat16)
    return lax.psum_scatter(
        jnp.dot(hidden, down_local, preferred_element_type=jnp.float32).astype(jnp.bfloat16),
        "tp",
        scatter_dimension=0,
        tiled=True,
    )


def moe_block(rows_in, targets, gate_values, w_in, w_down, expert_count, per_slot):
    tok_rows, top_count = targets.shape
    row_width = rows_in.shape[1]
    buffer, slot_index = pack_rows(rows_in, targets, expert_count, per_slot)
    arrived = to_experts(buffer, expert_count, per_slot)
    produced = run_expert(arrived, w_in, w_down)
    returned = to_owners(produced, expert_count, per_slot)
    picked = returned[slot_index].reshape(tok_rows, top_count, row_width)
    return jnp.sum(gate_values[:, :, None] * picked.astype(jnp.float32), axis=1)


def shards(
    tokens,
    experts_one,
    gates_one,
    w_in_one,
    w_down_one,
    norm_gain,
    experts_two,
    gates_two,
    placement_two,
    w_in_two,
    w_down_two,
):
    tok_rows, top_count = experts_one.shape
    expert_count = placement_two.shape[0]
    per_slot = capacity(tok_rows, top_count, expert_count)
    moe_one = moe_block(
        tokens, experts_one, gates_one, w_in_one, w_down_one, expert_count, per_slot
    )
    mixed = (tokens.astype(jnp.float32) + moe_one).astype(jnp.bfloat16)
    mixed = lax.optimization_barrier(mixed)
    mixed_wide = mixed.astype(jnp.float32)
    inv_rms = lax.rsqrt(jnp.mean(mixed_wide * mixed_wide, axis=1, keepdims=True) + 1e-06)
    normed = (mixed_wide * inv_rms * norm_gain[None, :]).astype(jnp.bfloat16)
    expert_range = jnp.arange(expert_count, dtype=jnp.int32)
    matches = experts_two[:, :, None] == expert_range[None, None, :]
    layer_slots = jnp.sum(jnp.where(matches, placement_two[None, None, :], 0), axis=2)
    moe_two = moe_block(
        normed, layer_slots, gates_two, w_in_two, w_down_two, expert_count, per_slot
    )
    return (mixed_wide + moe_two).astype(jnp.bfloat16)


def solution(mesh):
    in_specs = (
        P(("groups", "ep", "dp", "tp"), None),
        P(("groups", "ep", "dp", "tp"), None),
        P(("groups", "ep", "dp", "tp"), None),
        P(("ep", "dp"), None, None, "tp"),
        P(("ep", "dp"), "tp", None),
        P(),
        P(("groups", "ep", "dp", "tp"), None),
        P(("groups", "ep", "dp", "tp"), None),
        P(),
        P(("ep", "dp"), None, None, "tp"),
        P(("ep", "dp"), "tp", None),
    )
    out_specs = P(("groups", "ep", "dp", "tp"), None)
    ready = mesh.shape["tp"] == 1 and mesh.shape["dp"] == 4 and mesh.shape["ep"] == 4

    def body(*arrays):
        return (fused_shards if ready and arrays[0].shape[0] % 32 == 0 else shards)(*arrays)

    return jax.shard_map(body, mesh=mesh, in_specs=in_specs, out_specs=out_specs, check_vma=False)
```
